256 devices in a mesh: tx: 8 (over x_lo, y), ty: 8 (over z), lev: 4 (over x_hi, core).
Axes of the slice: x: 4 (x_hi: 2, x_lo: 2; x = x_hi * 2 + x_lo), y: 4, z: 8, core: 2. Of those that a mesh axis runs over, the one named last changes fastest.
Arguments:
- members: bfloat16 [8, 512, 128, 128], P('lev', 'tx', 'ty'), may hold values from -6 to 6
- obs_pert: bfloat16 [65536, 128], P(('tx', 'ty', 'lev')), may hold values from -6 to 6
- innovation: bfloat16 [65536], P(('tx', 'ty', 'lev')), may hold values from -6 to 6
- obs_precision: bfloat16 [65536], P(('tx', 'ty', 'lev')), may hold values from 0.25 to 4
- obs_owner: int32 [32, 8, 256], P('tx', 'ty'), may hold values from 0 to 63, as said below
- obs_slot: int32 [32, 8, 256], P('tx', 'ty'), may hold values from 0 to 1023
- obs_count: int32 [32, 8], P('tx', 'ty'), may hold values from 64 to 256
- local_weight: float32 [32, 8, 256], P('tx', 'ty'), may hold values from 0.05 to 1
Outputs:
- analysis: bfloat16 [8, 512, 128, 128], P('lev', 'tx', 'ty')
The draws below stay inside these ranges and needn't reach their ends.
Inputs may be any that keep to these rules, and one draw needn't show every extreme that they name: `obs_owner`: the tile numbered tx index times the number of ty tiles plus ty index; it is the coarse column's own tile or one of the tiles beside it, diagonals included. `obs_count`: slots at and beyond a coarse column's count are padding.
All inputs are finite; a program needn't handle non-finite values.
Results may differ from the reference program's by a relative error of at most 0.0054.
Values may be sent and summed in bfloat16 or wider, within the bound.
A program may use at most 64 MiB of HBM per device.

```python
import math
import jax
import jax.numpy as jnp
from jax import lax

K = 128
L = 256
SPACING = 16
NS_STEPS = 4
CX = 64
CY = 16
NX = 512
NY = 128
LEVELS = 8
NCX = 32
NCY = 8
OBS_TILE = 1024
NOBS = 65536


def draw_obs_owner(key, part):
    key_x, key_y = jax.random.split(jax.random.fold_in(key, 11))
    grid_shape = (NCX, NCY, L)
    step_x = jax.random.randint(key_x, grid_shape, -1, 2)
    step_y = jax.random.randint(key_y, grid_shape, -1, 2)
    tiles_x = NX // CX
    tiles_y = NY // CY
    home_x = (jnp.arange(NCX) // (CX // SPACING))[:, None, None]
    home_y = (jnp.arange(NCY) // (CY // SPACING))[None, :, None]
    owner_x = jnp.clip(home_x + step_x, 0, tiles_x - 1)
    owner_y = jnp.clip(home_y + step_y, 0, tiles_y - 1)
    return (owner_x * tiles_y + owner_y).astype(jnp.int32)


def with_ends(result, stream_key, smallest, high):
    spot = [jax.random.randint(jax.random.fold_in(stream_key, axis), (), 0, length) for axis, length in enumerate(result.shape)]
    longest = result.shape.index(max(result.shape))
    beside = spot[:longest] + [(spot[longest] + 1) % result.shape[longest]] + spot[longest + 1:]
    return result.at[tuple(spot)].set(smallest).at[tuple(beside)].set(high)


def shard_levels(own_key, dims, cuts, least, top_value):
    def one(position, parts):
        steps = jax.random.uniform(jax.random.fold_in(jax.random.fold_in(own_key, 6), position), (parts,), jnp.float32, least / len(cuts), top_value / len(cuts))
        return jnp.repeat(jnp.exp(steps), dims[position] // parts).reshape((-1,) + (1,) * (len(dims) - position - 1))

    factor_of = one(*cuts[0])
    for cut in cuts[1:]:
        factor_of = factor_of * one(*cut)
    return factor_of


def centred(stream_key, extent, scale, most, shards=(), kind=jnp.bfloat16):
    result = jax.random.normal(stream_key, extent, jnp.float32) * scale
    if len(shards) > 0:
        result = shard_levels(stream_key, extent, shards, -0.22, 0.18) * result
    return jnp.clip(result, min=-most, max=most).astype(kind)


def setup_inputs(seed: int = 0) -> dict:
    keys = jax.random.split(jax.random.key(seed), 9)
    return {
        "members": centred(keys[0], (LEVELS, NX, NY, K), 1.0, 6.0, ((0, 4), (1, 8), (2, 8))),
        "obs_pert": centred(keys[1], (NOBS, K), 1.0, 6.0, ((0, 256),)),
        "innovation": centred(keys[2], (NOBS,), 1.0, 6.0, ((0, 256),)),
        "obs_precision": jnp.clip(jnp.exp(math.log(4.0) - 2.7725887 * jax.random.uniform(keys[3], (NOBS,), jnp.float32) ** shard_levels(keys[3], (NOBS,), ((0, 256),), -0.2, 0.2)), 0.25, 4.0).astype(jnp.bfloat16),
        "obs_owner": draw_obs_owner(jax.random.fold_in(keys[8], 71), 0),
        "obs_slot": with_ends(jax.random.randint(keys[5], (NCX, NCY, L), 0, OBS_TILE), jax.random.fold_in(keys[5], 1), 0, OBS_TILE - 1).astype(jnp.int32),
        "obs_count": with_ends(jax.random.randint(keys[6], (NCX, NCY), L // 4, L + 1), jax.random.fold_in(keys[6], 1), L // 4, L).astype(jnp.int32),
        "local_weight": jnp.clip(0.05 + 0.95 * jax.random.uniform(keys[7], (NCX, NCY, L), jnp.float32) ** shard_levels(keys[7], (NCX, NCY, L), ((0, 8), (1, 8)), -0.2, 0.2), 0.05, 1.0),
    }


def finish_solve(gram_matrix, projected):
    member_count = gram_matrix.shape[1]
    spread = float(member_count - 1)
    identity = jnp.eye(member_count, dtype=jnp.float32)
    scale_norm = spread + jnp.sqrt(lax.optimization_barrier(jnp.sum(gram_matrix * gram_matrix, axis=(1, 2))))
    sqrt_iter = (spread * identity + gram_matrix) / scale_norm[:, None, None]
    inv_iter = jnp.broadcast_to(identity, sqrt_iter.shape)
    for iteration in range(NS_STEPS):
        middle = 1.5 * identity - 0.5 * jnp.einsum('bij,bjk->bik', inv_iter, sqrt_iter, precision=lax.Precision.HIGHEST)
        sqrt_iter = jnp.einsum('bij,bjk->bik', sqrt_iter, middle, precision=lax.Precision.HIGHEST)
        inv_iter = jnp.einsum('bij,bjk->bik', middle, inv_iter, precision=lax.Precision.HIGHEST)
    inner = jnp.einsum('bij,bj->bi', inv_iter, projected, precision=lax.Precision.HIGHEST)
    mean_weights = jnp.einsum('bij,bj->bi', inv_iter, inner, precision=lax.Precision.HIGHEST) / scale_norm[:, None]
    transform = (jnp.sqrt(spread) / jnp.sqrt(scale_norm))[:, None, None] * inv_iter + mean_weights[:, :, None]
    return transform.astype(jnp.bfloat16)

def fractions(count, half_span):
    place = jnp.arange(count)[:, None]
    within = jnp.arange(half_span)[None, :].astype(jnp.float32)
    return jnp.where(place % 2 == 0, (within + half_span + 0.5) / (2 * half_span), (within + 0.5) / (2 * half_span))

def reference(members, obs_pert, innovation, obs_precision, obs_owner, obs_slot, obs_count, local_weight):
    member_count = members.shape[3]
    slots = obs_owner.shape[2]
    lookup = obs_owner * OBS_TILE + obs_slot
    active = jnp.arange(slots)[None, None, :] < obs_count[:, :, None]

    def solve_strip(strip):
        strip_rows, strip_active, strip_local = strip
        pert_rows = obs_pert[strip_rows].astype(jnp.float32)
        precision_w = jnp.where(strip_active, obs_precision[strip_rows].astype(jnp.float32) * strip_local, 0.0)
        departure = innovation[strip_rows].astype(jnp.float32)
        gram_matrix = jnp.einsum('bsk,bsm->bkm', pert_rows * precision_w[:, :, None], pert_rows, precision=lax.Precision.HIGHEST)
        projected = jnp.einsum('bsk,bs->bk', pert_rows, precision_w * departure, precision=lax.Precision.HIGHEST)
        return finish_solve(gram_matrix, projected)
    weights = lax.map(solve_strip, (lookup, active, local_weight))
    padded = jnp.pad(weights, ((1, 1), (1, 1), (0, 0), (0, 0)), mode='edge')
    doubled = jnp.repeat(jnp.repeat(padded, 2, axis=0), 2, axis=1)
    half_span = SPACING // 2
    patch_x = NX // half_span
    patch_y = NY // half_span
    frac_x = fractions(patch_x, half_span)
    frac_y = fractions(patch_y, half_span)

    def one_level(level_states):
        states = level_states.astype(jnp.float32)
        ens_mean = lax.optimization_barrier(jnp.mean(states, axis=2, keepdims=True))
        pert = (states - ens_mean).astype(jnp.bfloat16)
        patched = pert.astype(jnp.float32).reshape(patch_x, half_span, patch_y, half_span, member_count)
        summed = jnp.zeros(patched.shape, jnp.float32)
        for upper_x in range(2):
            for upper_y in range(2):
                corner = doubled[1 + 2 * upper_x:1 + 2 * upper_x + patch_x, 1 + 2 * upper_y:1 + 2 * upper_y + patch_y].astype(jnp.float32)
                product = jnp.einsum('xaybi,xyij->xaybj', patched, corner)
                factor_x = frac_x if upper_x == 1 else 1.0 - frac_x
                factor_y = frac_y if upper_y == 1 else 1.0 - frac_y
                summed = summed + product * factor_x[:, :, None, None, None] * factor_y[None, None, :, :, None]
        return (ens_mean + summed.reshape(states.shape)).astype(jnp.bfloat16)
    return lax.map(one_level, members)
```

```python
import functools

import jax
import jax.numpy as jnp
from jax import lax
from jax.experimental import pallas as pl
from jax.experimental.pallas import tpu as pltpu
from jax.sharding import PartitionSpec as P

SPACING = 16
NS_STEPS = 4
MESH = pl.DeviceIdType.MESH
F32 = jnp.float32
BF16 = jnp.bfloat16
NT = (((1,), (1,)), ((), ()))

STEPS = ((0, 1), (0, -1), (1, 0), (-1, 0), (1, 1), (1, -1), (-1, 1), (-1, -1))


def halves(value):
    high = value.astype(BF16)
    return high, (value - high.astype(F32)).astype(BF16)


def product(left, right):
    left_high, left_low = left
    right_high, right_low = right
    return jnp.dot(
        jnp.concatenate([left_high, left_high, left_low], axis=1),
        jnp.concatenate([right_high, right_low, right_high], axis=0),
        preferred_element_type=F32,
    )


def solve(gram, proj_rows):
    members = gram.shape[0]
    spread = float(members - 1)
    rows = lax.broadcasted_iota(jnp.int32, gram.shape, 0)
    columns = lax.broadcasted_iota(jnp.int32, gram.shape, 1)
    diagonal = rows == columns
    square = jnp.sum(jnp.sum(gram * gram, axis=0, keepdims=True), axis=1, keepdims=True)
    norm = spread + jnp.sqrt(square)
    base = (jnp.where(diagonal, spread, 0.0) + gram) * (1.0 / norm)
    middle = jnp.where(diagonal, 1.5, 0.0) - 0.5 * base
    split_middle = halves(middle)
    root = product(halves(base), split_middle)
    inverse = middle
    target = jnp.broadcast_to(proj_rows[0:1, :], gram.shape).T
    for step in range(1, NS_STEPS):
        split_inverse = halves(inverse)
        split_root = halves(root)
        middle = jnp.where(diagonal, 1.5, 0.0) - 0.5 * product(split_inverse, split_root)
        split_middle = halves(middle)
        if step < NS_STEPS - 1:
            root = product(split_root, split_middle)
        else:
            target = product(split_inverse, halves(target))
        inverse = product(split_middle, split_inverse)
    inner = product(split_middle, halves(target))
    mean_weights = product(halves(inverse), halves(inner)) * (1.0 / norm)
    transform = (jnp.sqrt(spread) * lax.rsqrt(norm)) * inverse + mean_weights
    return transform.astype(BF16)


def kernel(
    tiles_x,
    tiles_y,
    members_ref,
    obs_ref,
    innovation_ref,
    precision_ref,
    owner_ref,
    slot_ref,
    count_ref,
    local_ref,
    out_ref,
    members_v,
    pert_v,
    mean_v,
    obs_v,
    near_v,
    scalar_v,
    owner_v,
    slot_v,
    count_v,
    local_v,
    dense_v,
    gram_v,
    from_core_v,
    sum_v,
    from_chip_v,
    weights_v,
    load_sem,
    obs_send,
    obs_recv,
    scalar_send,
    scalar_recv,
    gram_send,
    gram_recv,
    weight_send,
    weight_recv,
    pass_send,
    pass_recv,
):
    tx = lax.axis_index("tx")
    ty = lax.axis_index("ty")
    lev = lax.axis_index("lev")
    core = lev % 2
    own_obs, member_count = obs_ref.shape
    blocks = own_obs // 128
    columns = owner_ref.shape[0]
    slots = owner_ref.shape[2]

    def exists(dx, dy):
        x, y = tx + dx, ty + dy
        return (x >= 0) & (x < tiles_x) & (y >= 0) & (y < tiles_y)

    loads = [
        pltpu.make_async_copy(source, target, load_sem.at[k])
        for k, (source, target) in enumerate(
            (
                (obs_ref, obs_v),
                (owner_ref, owner_v),
                (slot_ref, slot_v),
                (count_ref, count_v),
                (local_ref, local_v),
                (precision_ref, scalar_v.at[4, 0]),
                (innovation_ref, scalar_v.at[4, 1]),
                (members_ref, members_v),
            )
        )
    ]
    for load in loads:
        load.start()

    barrier = pltpu.get_barrier_semaphore()
    other_core = (tx, ty, lev + 1 - 2 * core)
    other_chip = (tx, ty, (lev + 2) % 4)
    for dx, dy in STEPS:

        @pl.when(exists(dx, dy))
        def _():
            pl.semaphore_signal(
                barrier, inc=1, device_id=(tx + dx, ty + dy, lev), device_id_type=MESH
            )

    pl.semaphore_signal(barrier, inc=1, device_id=other_core, device_id_type=MESH)
    pl.semaphore_signal(barrier, inc=1, device_id=other_chip, device_id_type=MESH)

    loads[0].wait()
    near_v[4] = obs_v[...].astype(F32).T.astype(BF16)
    for load in loads[1:7]:
        load.wait()

    reach_x = 1 + (tx > 0).astype(jnp.int32) + (tx < tiles_x - 1).astype(jnp.int32)
    reach_y = 1 + (ty > 0).astype(jnp.int32) + (ty < tiles_y - 1).astype(jnp.int32)
    pl.semaphore_wait(barrier, reach_x * reach_y - 1 + 2)

    def obs_copies(dx, dy):
        theirs = (1 - dx) * 3 + (1 - dy)
        return tuple(
            pltpu.make_async_remote_copy(
                src_ref=buffer.at[4],
                dst_ref=buffer.at[theirs],
                send_sem=send.at[theirs],
                recv_sem=recv.at[theirs],
                device_id=(tx + dx, ty + dy, lev),
                device_id_type=MESH,
            )
            for buffer, send, recv in (
                (scalar_v, scalar_send, scalar_recv),
                (near_v, obs_send, obs_recv),
            )
        )

    for dx, dy in STEPS:

        @pl.when(exists(dx, dy))
        def _():
            for copy in obs_copies(dx, dy):
                copy.start()

    keys, lanes, parts = [], [], []
    position = lax.broadcasted_iota(jnp.int32, (1, slots), 1)
    quarter = own_obs
    for c in range(columns):
        owner = owner_v[c]
        slot = slot_v[c]
        near_x = owner // tiles_y - tx + 1
        near_y = owner % tiles_y - ty + 1
        block = (near_x * 3 + near_y) * blocks + (slot % quarter) // 128
        live = (position < count_v[c : c + 1, :]) & (slot // quarter == lev)
        keys.append(jnp.where(live, block * 8 + c, -1))
        lanes.append(slot % 128)
        parts.append(local_v[c])
    key = jnp.concatenate(keys, axis=1)
    lane = jnp.concatenate(lanes, axis=1)
    local = jnp.concatenate(parts, axis=1)
    high = local.astype(BF16).astype(F32)
    middle = (local - high).astype(BF16).astype(F32)
    low = local - high - middle
    dense_rows = 9 * blocks * 8
    row = lax.broadcasted_iota(jnp.int32, (dense_rows, columns * slots), 0)
    chosen = row == key
    spot = (lax.broadcasted_iota(jnp.int32, (128, columns * slots), 0) == lane).astype(F32)
    spot = spot.astype(BF16)
    dense = 0.0
    for part in (low, middle, high):
        dense += lax.dot_general(
            jnp.where(chosen, part, 0.0).astype(BF16), spot, NT, preferred_element_type=F32
        )
    dense_v[...] = dense.reshape(9 * blocks, 8, 128)

    gram_v[...] = jnp.zeros_like(gram_v)

    def add_block(near):
        turned = near_v[near]
        wide = turned.astype(F32)
        scalars = scalar_v[near].astype(F32)
        weight = jnp.concatenate(
            [dense_v[near * blocks + h] * scalars[0, h : h + 1, :] for h in range(blocks)], axis=1
        )
        departure = jnp.concatenate([scalars[1, h : h + 1, :] for h in range(blocks)], axis=1)
        for c in range(columns):
            upper, lower = halves(wide * weight[c : c + 1, :])
            gram_v[c, 0:member_count, :] += lax.dot_general(
                upper, turned, NT, preferred_element_type=F32
            ) + lax.dot_general(lower, turned, NT, preferred_element_type=F32)
        upper, lower = halves(weight * departure)
        shares = lax.dot_general(
            upper, turned, NT, preferred_element_type=F32
        ) + lax.dot_general(lower, turned, NT, preferred_element_type=F32)
        for c in range(columns):
            gram_v[c, member_count : member_count + 8, :] += jnp.broadcast_to(
                shares[c : c + 1, :], (8, member_count)
            )

    add_block(4)

    loads[7].wait()
    averaging = jnp.full((member_count, member_count), 1.0 / member_count, BF16)
    level_count, width_x, width_y, _ = members_v.shape
    for level in range(level_count):
        for first in range(0, width_x, 32):
            states = members_v[level, first : first + 32].reshape(32 * width_y, member_count)
            mean = jnp.dot(states, averaging, preferred_element_type=F32)
            mean_v[level, first : first + 32] = mean.reshape(32, width_y, member_count)
            pert_v[level, first : first + 32] = (
                (states.astype(F32) - mean).astype(BF16).reshape(32, width_y, member_count)
            )

    for dx, dy in STEPS:

        @pl.when(exists(dx, dy))
        def _():
            near = (1 + dx) * 3 + (1 + dy)
            for copy in obs_copies(-dx, -dy):
                copy.wait_recv()
            add_block(near)

    mine, others = 2 * core, 2 - 2 * core
    to_core = pltpu.make_async_remote_copy(
        src_ref=gram_v.at[pl.ds(others, 2)],
        dst_ref=from_core_v,
        send_sem=gram_send.at[0],
        recv_sem=gram_recv.at[0],
        device_id=other_core,
        device_id_type=MESH,
    )
    to_core.start()
    to_core.wait_recv()
    sum_v[...] = gram_v[pl.ds(mine, 2)] + from_core_v[...]
    to_chip = pltpu.make_async_remote_copy(
        src_ref=sum_v,
        dst_ref=from_chip_v,
        send_sem=gram_send.at[1],
        recv_sem=gram_recv.at[1],
        device_id=other_chip,
        device_id_type=MESH,
    )
    to_chip.start()
    to_chip.wait_recv()
    for k in range(2):
        gram = sum_v[k, 0:member_count] + from_chip_v[k, 0:member_count]
        proj = sum_v[k, member_count:] + from_chip_v[k, member_count:]
        weights_v[1, 1 + mine + k] = solve(gram, proj)

    outward = 2 * core - 1
    rim_from = 1 + 3 * core
    rim_to = 5 - 5 * core

    def pass_copy(index, ref):
        return pltpu.make_async_remote_copy(
            src_ref=ref,
            dst_ref=ref,
            send_sem=pass_send.at[index],
            recv_sem=pass_recv.at[index],
            device_id=other_core,
            device_id_type=MESH,
        )

    def pair(y, first):
        return weights_v.at[y, pl.ds(first, 2)]

    pair_mine, pair_other = 1 + mine, 1 + others
    rim_mine, rim_other = rim_to, 5 - rim_to

    def pair_copy(e):
        return pltpu.make_async_remote_copy(
            src_ref=pair(1, pair_mine),
            dst_ref=pair(1 - e, pair_mine),
            send_sem=weight_send.at[1 - e],
            recv_sem=weight_recv.at[1 - e],
            device_id=(tx, ty + e, lev),
            device_id_type=MESH,
        )

    def rim_copy(e, sign):
        return pltpu.make_async_remote_copy(
            src_ref=weights_v.at[1, rim_from],
            dst_ref=weights_v.at[1 - e, rim_mine],
            send_sem=weight_send.at[4 - e],
            recv_sem=weight_recv.at[4 - e],
            device_id=(tx + sign * outward, ty + e, lev),
            device_id_type=MESH,
        )

    for e in (1, -1):

        @pl.when(exists(0, e))
        def _():
            pair_copy(e).start()

    for e in (1, -1, 0):

        @pl.when(exists(outward, e))
        def _():
            rim_copy(e, 1).start()

    pass_copy(1, pair(1, pair_mine)).start()
    for e in (0, 1, -1):
        if e:

            @pl.when(exists(0, -e))
            def _():
                pair_copy(e).wait_recv()
                pass_copy(1 - e, pair(1 - e, pair_mine)).start()

        @pl.when(exists(-outward, -e))
        def _():
            rim_copy(e, 1).wait_recv()
            pass_copy(4 - e, weights_v.at[1 - e, rim_mine]).start()

    pass_copy(1, pair(1, pair_other)).wait_recv()
    for e in (0, 1, -1):
        if e:

            @pl.when(exists(0, -e))
            def _():
                pass_copy(1 - e, pair(1 - e, pair_other)).wait_recv()

        @pl.when(exists(outward, -e))
        def _():
            pass_copy(4 - e, weights_v.at[1 - e, rim_other]).wait_recv()

    half_span = SPACING // 2
    places_y = [jnp.where(ty == 0, 1, 0), 1, jnp.where(ty == tiles_y - 1, 1, 2)]
    places_x = [jnp.where(tx == 0, 1, 0), 1, 2, 3, 4, jnp.where(tx == tiles_x - 1, 4, 5)]
    within = lax.broadcasted_iota(jnp.int32, (half_span, member_count), 0).astype(F32)
    upper_y = [(within + half_span + 0.5) / SPACING, (within + 0.5) / SPACING]
    for patch in range(width_x // half_span):
        left = (patch + 1) // 2
        corners = jnp.concatenate(
            [weights_v[y, x] for x in (places_x[left], places_x[left + 1]) for y in places_y],
            axis=1,
        )
        first = patch * half_span
        pert = pert_v[:, first : first + half_span].reshape(-1, member_count)
        mixed = jnp.dot(pert, corners, preferred_element_type=F32)
        mixed = mixed.reshape(level_count, half_span, width_y, 6 * member_count)
        for level in range(level_count):
            for x in range(half_span):
                fx = (x + 0.5 + (half_span if patch % 2 == 0 else 0)) / SPACING
                sides = []
                for p in range(2):
                    fy = upper_y[p]
                    rows = mixed[level, x, p * half_span : (p + 1) * half_span]
                    total = mean_v[level, first + x, p * half_span : (p + 1) * half_span]
                    for u in range(2):
                        for v in range(2):
                            at = (u * 3 + p + v) * member_count
                            factor = (fx if u else 1.0 - fx) * (fy if v else 1.0 - fy)
                            total = total + rows[:, at : at + member_count] * factor
                    sides.append(total)
                out_ref[level, first + x] = jnp.concatenate(sides, axis=0).astype(BF16)

    for dx, dy in STEPS:

        @pl.when(exists(dx, dy))
        def _():
            for copy in obs_copies(dx, dy):
                copy.wait_send()

    to_core.wait_send()
    to_chip.wait_send()
    pass_copy(1, pair(1, pair_mine)).wait_send()
    for e in (0, 1, -1):
        if e:

            @pl.when(exists(0, e))
            def _():
                pair_copy(e).wait_send()

            @pl.when(exists(0, -e))
            def _():
                pass_copy(1 - e, pair(1 - e, pair_mine)).wait_send()

        @pl.when(exists(outward, e))
        def _():
            rim_copy(e, 1).wait_send()

        @pl.when(exists(-outward, -e))
        def _():
            pass_copy(4 - e, weights_v.at[1 - e, rim_mine]).wait_send()


def per_device(
    tiles_x,
    tiles_y,
    members,
    obs_pert,
    innovation,
    obs_precision,
    obs_owner,
    obs_slot,
    obs_count,
    local_weight,
):
    own_obs, member_count = obs_pert.shape
    blocks = own_obs // 128
    anywhere = pl.BlockSpec(memory_space=pl.ANY)
    dma = pltpu.SemaphoreType.DMA
    return pl.pallas_call(
        functools.partial(kernel, tiles_x, tiles_y),
        out_shape=jax.ShapeDtypeStruct(members.shape, BF16),
        in_specs=[anywhere] * 8,
        out_specs=pl.BlockSpec(memory_space=pltpu.VMEM),
        scratch_shapes=[
            pltpu.VMEM(members.shape, BF16),
            pltpu.VMEM(members.shape, BF16),
            pltpu.VMEM(members.shape, F32),
            pltpu.VMEM(obs_pert.shape, BF16),
            pltpu.VMEM((9, member_count, own_obs), BF16),
            pltpu.VMEM((9, 2, blocks, 128), BF16),
            pltpu.VMEM(obs_owner.shape, jnp.int32),
            pltpu.VMEM(obs_slot.shape, jnp.int32),
            pltpu.VMEM(obs_count.shape, jnp.int32),
            pltpu.VMEM(local_weight.shape, F32),
            pltpu.VMEM((9 * blocks, 8, 128), F32),
            pltpu.VMEM((4, member_count + 8, member_count), F32),
            pltpu.VMEM((2, member_count + 8, member_count), F32),
            pltpu.VMEM((2, member_count + 8, member_count), F32),
            pltpu.VMEM((2, member_count + 8, member_count), F32),
            pltpu.VMEM((3, 6, member_count, member_count), BF16),
            dma((8,)),
            dma((9,)),
            dma((9,)),
            dma((9,)),
            dma((9,)),
            dma((2,)),
            dma((2,)),
            dma((6,)),
            dma((6,)),
            dma((6,)),
            dma((6,)),
        ],
        compiler_params=pltpu.CompilerParams(
            collective_id=0, has_side_effects=True, vmem_limit_bytes=48 * 1024 * 1024
        ),
    )(
        members,
        obs_pert,
        innovation.reshape(blocks, 128),
        obs_precision.reshape(blocks, 128),
        obs_owner,
        obs_slot,
        obs_count,
        local_weight,
    )


def solution(mesh):
    placed = (
        P("lev", "tx", "ty", None),
        P(("tx", "ty", "lev"), None),
        P(("tx", "ty", "lev")),
        P(("tx", "ty", "lev")),
        P("tx", "ty", None),
        P("tx", "ty", None),
        P("tx", "ty"),
        P("tx", "ty", None),
    )
    return jax.shard_map(
        functools.partial(per_device, mesh.shape["tx"], mesh.shape["ty"]),
        mesh=mesh,
        in_specs=placed,
        out_specs=P("lev", "tx", "ty", None),
        check_vma=False,
    )
```

```python
import functools

import jax
import jax.numpy as jnp
from jax import lax
from jax.experimental import pallas as pl
from jax.experimental.pallas import tpu as pltpu
from jax.sharding import PartitionSpec as P

SPACING = 16
NS_STEPS = 4
MESH = pl.DeviceIdType.MESH
F32 = jnp.float32
BF16 = jnp.bfloat16
NT = (((1,), (1,)), ((), ()))

STEPS = ((0, 1), (0, -1), (1, 0), (-1, 0), (1, 1), (1, -1), (-1, 1), (-1, -1))
GROUPS = (STEPS[:4], STEPS[4:])


def halves(value):
    high = value.astype(BF16)
    return high, (value - high.astype(F32)).astype(BF16)


def product(left, right):
    left_high, left_low = left
    right_high, right_low = right
    return jnp.dot(
        jnp.concatenate([left_high, left_high, left_low], axis=1),
        jnp.concatenate([right_high, right_low, right_high], axis=0),
        preferred_element_type=F32,
    )


def solve(gram, proj_rows):
    members = gram.shape[0]
    spread = float(members - 1)
    rows = lax.broadcasted_iota(jnp.int32, gram.shape, 0)
    columns = lax.broadcasted_iota(jnp.int32, gram.shape, 1)
    diagonal = rows == columns
    square = jnp.sum(jnp.sum(gram * gram, axis=0, keepdims=True), axis=1, keepdims=True)
    norm = spread + jnp.sqrt(square)
    raised = jnp.where(diagonal, spread, 0.0) + gram
    split_raised = halves(raised)
    squared = product(split_raised, split_raised)
    scale = 1.0 / norm
    base = raised * scale
    middle = jnp.where(diagonal, 1.5, 0.0) - 0.5 * base
    split_middle = halves(middle)
    root = 1.5 * base - squared * (0.5 * scale * scale)
    inverse = middle
    target = jnp.broadcast_to(proj_rows[0:1, :], gram.shape).T
    for step in range(1, NS_STEPS):
        split_inverse = halves(inverse)
        split_root = halves(root)
        middle = jnp.where(diagonal, 1.5, 0.0) - 0.5 * product(split_inverse, split_root)
        split_middle = halves(middle)
        if step < NS_STEPS - 1:
            root = product(split_root, split_middle)
        else:
            target = product(split_inverse, halves(target))
        inverse = product(split_middle, split_inverse)
    inner = product(split_middle, halves(target))
    mean_weights = product(halves(inverse), halves(inner)) * scale
    transform = (jnp.sqrt(spread) * lax.rsqrt(norm)) * inverse + mean_weights
    return transform.astype(BF16)


def kernel(
    tiles_x,
    tiles_y,
    members_ref,
    obs_ref,
    innovation_ref,
    precision_ref,
    owner_ref,
    slot_ref,
    count_ref,
    local_ref,
    out_ref,
    members_v,
    pert_v,
    mean_v,
    obs_v,
    near_v,
    scalar_v,
    owner_v,
    slot_v,
    count_v,
    local_v,
    dense_v,
    gram_v,
    from_core_v,
    sum_v,
    half_v,
    from_chip_v,
    weights_v,
    load_sem,
    obs_send,
    obs_recv,
    scalar_send,
    scalar_recv,
    gram_send,
    gram_recv,
    weight_send,
    weight_recv,
    pass_send,
    pass_recv,
):
    tx = lax.axis_index("tx")
    ty = lax.axis_index("ty")
    lev = lax.axis_index("lev")
    core = lev % 2
    own_obs, member_count = obs_ref.shape
    blocks = own_obs // 128
    columns = owner_ref.shape[0]
    slots = owner_ref.shape[2]

    def exists(dx, dy):
        x, y = tx + dx, ty + dy
        return (x >= 0) & (x < tiles_x) & (y >= 0) & (y < tiles_y)

    loads = [
        pltpu.make_async_copy(source, target, load_sem.at[k])
        for k, (source, target) in enumerate(
            (
                (obs_ref, obs_v),
                (owner_ref, owner_v),
                (slot_ref, slot_v),
                (count_ref, count_v),
                (local_ref, local_v),
                (precision_ref, scalar_v.at[4, 0]),
                (innovation_ref, scalar_v.at[4, 1]),
                (members_ref, members_v),
            )
        )
    ]
    for load in loads:
        load.start()

    barrier = pltpu.get_barrier_semaphore()
    other_core = (tx, ty, lev + 1 - 2 * core)
    other_chip = (tx, ty, (lev + 2) % 4)
    far_core = (tx, ty, 3 - lev)
    for dx, dy in STEPS:

        @pl.when(exists(dx, dy))
        def _():
            pl.semaphore_signal(
                barrier, inc=1, device_id=(tx + dx, ty + dy, lev), device_id_type=MESH
            )

    outward = 2 * core - 1
    for e in (-1, 0, 1):

        @pl.when(exists(outward, e))
        def _():
            pl.semaphore_signal(
                barrier,
                inc=1,
                device_id=(tx + outward, ty + e, lev + 1 - 2 * core),
                device_id_type=MESH,
            )

    pl.semaphore_signal(barrier, inc=1, device_id=other_core, device_id_type=MESH)
    pl.semaphore_signal(barrier, inc=1, device_id=other_chip, device_id_type=MESH)
    pl.semaphore_signal(barrier, inc=1, device_id=far_core, device_id_type=MESH)

    for dx, dy in STEPS:

        @pl.when(jnp.logical_not(exists(dx, dy)))
        def _():
            near = (1 + dx) * 3 + (1 + dy)
            near_v[near] = jnp.zeros(near_v.shape[1:], BF16)
            scalar_v[near] = jnp.zeros(scalar_v.shape[1:], BF16)

    loads[0].wait()
    near_v[4] = obs_v[...].astype(F32).T.astype(BF16)
    for load in loads[1:7]:
        load.wait()

    reach_x = 1 + (tx > 0).astype(jnp.int32) + (tx < tiles_x - 1).astype(jnp.int32)
    reach_y = 1 + (ty > 0).astype(jnp.int32) + (ty < tiles_y - 1).astype(jnp.int32)
    crossing = exists(outward, 0).astype(jnp.int32) * reach_y
    pl.semaphore_wait(barrier, reach_x * reach_y - 1 + crossing + 3)

    def obs_copies(dx, dy):
        theirs = (1 - dx) * 3 + (1 - dy)
        return tuple(
            pltpu.make_async_remote_copy(
                src_ref=buffer.at[4],
                dst_ref=buffer.at[theirs],
                send_sem=send.at[theirs],
                recv_sem=recv.at[theirs],
                device_id=(tx + dx, ty + dy, lev),
                device_id_type=MESH,
            )
            for buffer, send, recv in (
                (scalar_v, scalar_send, scalar_recv),
                (near_v, obs_send, obs_recv),
            )
        )

    for dx, dy in STEPS:

        @pl.when(exists(dx, dy))
        def _():
            for copy in obs_copies(dx, dy):
                copy.start()

    keys, lanes, parts = [], [], []
    position = lax.broadcasted_iota(jnp.int32, (1, slots), 1)
    quarter = own_obs
    for c in range(columns):
        owner = owner_v[c]
        slot = slot_v[c]
        near_x = owner // tiles_y - tx + 1
        near_y = owner % tiles_y - ty + 1
        block = (near_x * 3 + near_y) * blocks + (slot % quarter) // 128
        live = (position < count_v[:, c : c + 1]) & (slot // quarter == lev)
        keys.append(jnp.where(live, block * 8 + c, -1))
        lanes.append(slot % 128)
        parts.append(local_v[c])
    key = jnp.concatenate(keys, axis=1)
    lane = jnp.concatenate(lanes, axis=1)
    local = jnp.concatenate(parts, axis=1)
    high = local.astype(BF16).astype(F32)
    middle = (local - high).astype(BF16).astype(F32)
    low = local - high - middle
    dense_rows = 9 * blocks * 8
    row = lax.broadcasted_iota(jnp.int32, (dense_rows, columns * slots), 0)
    chosen = row == key
    spot = (lax.broadcasted_iota(jnp.int32, (128, columns * slots), 0) == lane).astype(F32)
    spot = spot.astype(BF16)
    dense = 0.0
    for part in (low, middle, high):
        dense += lax.dot_general(
            jnp.where(chosen, part, 0.0).astype(BF16), spot, NT, preferred_element_type=F32
        )
    dense_v[...] = dense.reshape(9 * blocks, 8, 128)

    gram_v[...] = jnp.zeros_like(gram_v)

    def add_blocks(nears):
        left, right = [], []
        for near in nears:
            turned = near_v[near]
            wide = turned.astype(F32)
            scalars = scalar_v[near].astype(F32)
            weight = jnp.concatenate(
                [dense_v[near * blocks + h] * scalars[0, h : h + 1, :] for h in range(blocks)],
                axis=1,
            )
            departure = jnp.concatenate([scalars[1, h : h + 1, :] for h in range(blocks)], axis=1)
            pairs = [halves(wide * weight[c : c + 1, :]) for c in range(columns)]
            pairs.append(halves(weight * departure))
            left.append(jnp.concatenate([half for pair in pairs for half in pair], axis=0))
            right.append(turned)
        sums = lax.dot_general(
            jnp.concatenate(left, axis=1),
            jnp.concatenate(right, axis=1),
            NT,
            preferred_element_type=F32,
        )
        at = 0
        for c in range(columns):
            gram_v[c, 0:member_count, :] += (
                sums[at : at + member_count] + sums[at + member_count : at + 2 * member_count]
            )
            at += 2 * member_count
        shares = sums[at : at + 8] + sums[at + 8 : at + 16]
        for c in range(columns):
            gram_v[c, member_count : member_count + 8, :] += jnp.broadcast_to(
                shares[c : c + 1, :], (8, member_count)
            )

    add_blocks([4])

    loads[7].wait()
    averaging = jnp.full((member_count, member_count), 1.0 / member_count, BF16)
    level_count, width_x, width_y, _ = members_v.shape
    for level in range(level_count):
        for first in range(0, width_x, 32):
            states = members_v[level, first : first + 32].reshape(32 * width_y, member_count)
            mean = jnp.dot(states, averaging, preferred_element_type=F32)
            mean_v[level, first : first + 32] = mean.reshape(32, width_y, member_count)
            pert_v[level, first : first + 32] = (
                (states.astype(F32) - mean).astype(BF16).reshape(32, width_y, member_count)
            )

    for group in GROUPS:
        for dx, dy in group:

            @pl.when(exists(dx, dy))
            def _():
                for copy in obs_copies(-dx, -dy):
                    copy.wait_recv()

        add_blocks([(1 + dx) * 3 + (1 + dy) for dx, dy in group])

    mine, others = 2 * core, 2 - 2 * core
    for c in range(columns):
        half_v[c, 0:member_count] = gram_v[c, 0:member_count].astype(BF16)
        half_v[c, member_count:] = jnp.concatenate(halves(gram_v[c, member_count:]), axis=0)

    def gram_copy(index, source, target, where):
        return pltpu.make_async_remote_copy(
            src_ref=source,
            dst_ref=target,
            send_sem=gram_send.at[index],
            recv_sem=gram_recv.at[index],
            device_id=where,
            device_id_type=MESH,
        )

    to_core = gram_copy(0, gram_v.at[pl.ds(others, 2)], from_core_v, other_core)
    to_chip = gram_copy(1, half_v.at[pl.ds(mine, 2)], from_chip_v.at[0], other_chip)
    to_far = gram_copy(2, half_v.at[pl.ds(others, 2)], from_chip_v.at[1], far_core)
    to_far.start()
    to_chip.start()
    to_core.start()
    to_core.wait_recv()
    sum_v[...] = gram_v[pl.ds(mine, 2)] + from_core_v[...]
    to_chip.wait_recv()
    to_far.wait_recv()
    for k in range(2):
        theirs = from_chip_v[0, k].astype(F32) + from_chip_v[1, k].astype(F32)
        gram = sum_v[k, 0:member_count] + theirs[0:member_count]
        upper = theirs[member_count : member_count + 8]
        lower = theirs[member_count + 8 : member_count + 16]
        proj = sum_v[k, member_count:] + (upper + lower)
        weights_v[1, 1 + mine + k] = solve(gram, proj)

    rim_from = 1 + 3 * core
    rim_to = 5 - 5 * core

    def pass_copy(index, ref):
        return pltpu.make_async_remote_copy(
            src_ref=ref,
            dst_ref=ref,
            send_sem=pass_send.at[index],
            recv_sem=pass_recv.at[index],
            device_id=other_core,
            device_id_type=MESH,
        )

    def pair(y, first):
        return weights_v.at[y, pl.ds(first, 2)]

    pair_mine, pair_other = 1 + mine, 1 + others
    rim_mine, rim_other = rim_to, 5 - rim_to

    def pair_copy(e):
        return pltpu.make_async_remote_copy(
            src_ref=pair(1, pair_mine),
            dst_ref=pair(1 - e, pair_mine),
            send_sem=weight_send.at[1 - e],
            recv_sem=weight_recv.at[1 - e],
            device_id=(tx, ty + e, lev),
            device_id_type=MESH,
        )

    def rim_copy(e, across):
        where = (tx + outward, ty + e, lev + across * (1 - 2 * core))
        index = 3 + 3 * across + 1 - e
        return pltpu.make_async_remote_copy(
            src_ref=weights_v.at[1, rim_from],
            dst_ref=weights_v.at[1 - e, rim_mine],
            send_sem=weight_send.at[index],
            recv_sem=weight_recv.at[index],
            device_id=where,
            device_id_type=MESH,
        )

    for e in (1, -1):

        @pl.when(exists(0, e))
        def _():
            pair_copy(e).start()

    for e in (1, -1, 0):

        @pl.when(exists(outward, e))
        def _():
            rim_copy(e, 0).start()
            rim_copy(e, 1).start()

    pass_copy(1, pair(1, pair_mine)).start()
    for e in (1, -1):

        @pl.when(exists(0, -e))
        def _():
            pair_copy(e).wait_recv()
            pass_copy(1 - e, pair(1 - e, pair_mine)).start()

    pass_copy(1, pair(1, pair_other)).wait_recv()
    for e in (1, -1):

        @pl.when(exists(0, -e))
        def _():
            pass_copy(1 - e, pair(1 - e, pair_other)).wait_recv()

    for e in (0, 1, -1):

        @pl.when(exists(-outward, -e))
        def _():
            rim_copy(e, 0).wait_recv()

        @pl.when(exists(outward, -e))
        def _():
            pltpu.make_async_remote_copy(
                src_ref=weights_v.at[1, rim_from],
                dst_ref=weights_v.at[1 - e, rim_other],
                send_sem=weight_send.at[7 - e],
                recv_sem=weight_recv.at[7 - e],
                device_id=other_core,
                device_id_type=MESH,
            ).wait_recv()

    half_span = SPACING // 2
    places_y = [jnp.where(ty == 0, 1, 0), 1, jnp.where(ty == tiles_y - 1, 1, 2)]
    places_x = [jnp.where(tx == 0, 1, 0), 1, 2, 3, 4, jnp.where(tx == tiles_x - 1, 4, 5)]
    within = lax.broadcasted_iota(jnp.int32, (half_span, member_count), 0).astype(F32)
    upper_y = [(within + half_span + 0.5) / SPACING, (within + 0.5) / SPACING]
    for patch in range(width_x // half_span):
        left = (patch + 1) // 2
        corners = jnp.concatenate(
            [weights_v[y, x] for x in (places_x[left], places_x[left + 1]) for y in places_y],
            axis=1,
        )
        first = patch * half_span
        pert = pert_v[:, first : first + half_span].reshape(-1, member_count)
        mixed = jnp.dot(pert, corners, preferred_element_type=F32)
        mixed = mixed.reshape(level_count, half_span, width_y, 6 * member_count)
        for level in range(level_count):
            for x in range(half_span):
                fx = (x + 0.5 + (half_span if patch % 2 == 0 else 0)) / SPACING
                sides = []
                for p in range(2):
                    fy = upper_y[p]
                    rows = mixed[level, x, p * half_span : (p + 1) * half_span]
                    total = mean_v[level, first + x, p * half_span : (p + 1) * half_span]
                    for u in range(2):
                        for v in range(2):
                            at = (u * 3 + p + v) * member_count
                            factor = (fx if u else 1.0 - fx) * (fy if v else 1.0 - fy)
                            total = total + rows[:, at : at + member_count] * factor
                    sides.append(total)
                out_ref[level, first + x] = jnp.concatenate(sides, axis=0).astype(BF16)

    for dx, dy in STEPS:

        @pl.when(exists(dx, dy))
        def _():
            for copy in obs_copies(dx, dy):
                copy.wait_send()

    to_core.wait_send()
    to_chip.wait_send()
    to_far.wait_send()
    pass_copy(1, pair(1, pair_mine)).wait_send()
    for e in (0, 1, -1):
        if e:

            @pl.when(exists(0, e))
            def _():
                pair_copy(e).wait_send()

            @pl.when(exists(0, -e))
            def _():
                pass_copy(1 - e, pair(1 - e, pair_mine)).wait_send()

        @pl.when(exists(outward, e))
        def _():
            rim_copy(e, 0).wait_send()
            rim_copy(e, 1).wait_send()


def per_device(
    tiles_x,
    tiles_y,
    members,
    obs_pert,
    innovation,
    obs_precision,
    obs_owner,
    obs_slot,
    obs_count,
    local_weight,
):
    own_obs, member_count = obs_pert.shape
    blocks = own_obs // 128
    anywhere = pl.BlockSpec(memory_space=pltpu.HBM)
    dma = pltpu.SemaphoreType.DMA
    return pl.pallas_call(
        functools.partial(kernel, tiles_x, tiles_y),
        out_shape=jax.ShapeDtypeStruct(members.shape, BF16),
        in_specs=[anywhere] * 8,
        out_specs=pl.BlockSpec(memory_space=pltpu.VMEM),
        scratch_shapes=[
            pltpu.VMEM(members.shape, BF16),
            pltpu.VMEM(members.shape, BF16),
            pltpu.VMEM(members.shape, F32),
            pltpu.VMEM(obs_pert.shape, BF16),
            pltpu.VMEM((9, member_count, own_obs), BF16),
            pltpu.VMEM((9, 2, blocks, 128), BF16),
            pltpu.VMEM(obs_owner.shape, jnp.int32),
            pltpu.VMEM(obs_slot.shape, jnp.int32),
            pltpu.VMEM((1, obs_count.size), jnp.int32),
            pltpu.VMEM(local_weight.shape, F32),
            pltpu.VMEM((9 * blocks, 8, 128), F32),
            pltpu.VMEM((4, member_count + 8, member_count), F32),
            pltpu.VMEM((2, member_count + 8, member_count), F32),
            pltpu.VMEM((2, member_count + 8, member_count), F32),
            pltpu.VMEM((4, member_count + 16, member_count), BF16),
            pltpu.VMEM((2, 2, member_count + 16, member_count), BF16),
            pltpu.VMEM((3, 6, member_count, member_count), BF16),
            dma((8,)),
            dma((9,)),
            dma((9,)),
            dma((9,)),
            dma((9,)),
            dma((3,)),
            dma((3,)),
            dma((9,)),
            dma((9,)),
            dma((3,)),
            dma((3,)),
        ],
        compiler_params=pltpu.CompilerParams(
            collective_id=0, has_side_effects=True, vmem_limit_bytes=48 * 1024 * 1024
        ),
    )(
        *(pltpu.with_memory_space_constraint(x, pltpu.HBM) for x in (
        members,
        obs_pert,
        innovation.reshape(blocks, 128),
        obs_precision.reshape(blocks, 128),
        obs_owner,
        obs_slot,
        obs_count.reshape(1, -1),
        local_weight,
        ))
    )


def solution(mesh):
    placed = (
        P("lev", "tx", "ty", None),
        P(("tx", "ty", "lev"), None),
        P(("tx", "ty", "lev")),
        P(("tx", "ty", "lev")),
        P("tx", "ty", None),
        P("tx", "ty", None),
        P("tx", "ty"),
        P("tx", "ty", None),
    )
    return jax.shard_map(
        functools.partial(per_device, mesh.shape["tx"], mesh.shape["ty"]),
        mesh=mesh,
        in_specs=placed,
        out_specs=P("lev", "tx", "ty", None),
        check_vma=False,
    )
```

```python
import functools

import jax
import jax.numpy as jnp
from jax import lax
from jax.experimental import pallas as pl
from jax.experimental.pallas import tpu as pltpu
from jax.sharding import PartitionSpec as P

SPACING = 16
NS_STEPS = 4
MESH = pl.DeviceIdType.MESH
F32 = jnp.float32
BF16 = jnp.bfloat16
NT = (((1,), (1,)), ((), ()))

STEPS = ((1, 1), (1, -1), (-1, 1), (-1, -1), (0, 1), (0, -1), (1, 0), (-1, 0))
GROUPS = (STEPS,)


def halves(value):
    high = value.astype(BF16)
    return high, (value - high.astype(F32)).astype(BF16)


def product(left, right):
    left_high, left_low = left
    right_high, right_low = right
    return jnp.dot(
        jnp.concatenate([left_high, left_high, left_low], axis=1),
        jnp.concatenate([right_high, right_low, right_high], axis=0),
        preferred_element_type=F32,
    )


def beside(left, right):
    return tuple(jnp.concatenate(pair, axis=1) for pair in zip(left, right))


def solve(gram, proj_rows):
    members = gram.shape[0]
    spread = float(members - 1)
    rows = lax.broadcasted_iota(jnp.int32, gram.shape, 0)
    columns = lax.broadcasted_iota(jnp.int32, gram.shape, 1)
    diagonal = rows == columns
    square = jnp.sum(jnp.sum(gram * gram, axis=0, keepdims=True), axis=1, keepdims=True)
    norm = spread + jnp.sqrt(square)
    raised = jnp.where(diagonal, spread, 0.0) + gram
    split_raised = halves(raised)
    squared = product(split_raised, split_raised)
    scale = 1.0 / norm
    base = raised * scale
    three_halves = jnp.where(diagonal, 1.5, 0.0)
    inverse = three_halves - 0.5 * base
    root = 1.5 * base - squared * (0.5 * scale * scale)
    target = jnp.broadcast_to(proj_rows[0:1, :], gram.shape).T
    for step in range(1, NS_STEPS):
        split_inverse, split_root = halves(inverse), halves(root)
        if step < NS_STEPS - 1:
            middle = three_halves - 0.5 * product(split_inverse, split_root)
            both = product(halves(middle), beside(split_root, split_inverse))
            root, inverse = both[:, :members], both[:, members:]
        else:
            both = product(split_inverse, beside(split_root, halves(target)))
            middle = three_halves - 0.5 * both[:, :members]
            both = product(halves(middle), beside(split_inverse, halves(both[:, members:])))
            inverse, inner = both[:, :members], both[:, members:]
    mean_weights = product(halves(inverse), halves(inner)) * scale
    transform = (jnp.sqrt(spread) * lax.rsqrt(norm)) * inverse + mean_weights
    return transform.astype(BF16)


def kernel(
    tiles_x,
    tiles_y,
    members_ref,
    obs_ref,
    innovation_ref,
    precision_ref,
    owner_ref,
    slot_ref,
    count_ref,
    local_ref,
    out_ref,
    members_v,
    pert_v,
    mean_v,
    obs_v,
    near_v,
    scalar_v,
    owner_v,
    slot_v,
    count_v,
    local_v,
    dense_v,
    gram_v,
    from_core_v,
    sum_v,
    half_v,
    from_chip_v,
    weights_v,
    load_sem,
    obs_send,
    obs_recv,
    scalar_send,
    scalar_recv,
    gram_send,
    gram_recv,
    weight_send,
    weight_recv,
    pass_send,
    pass_recv,
):
    tx = lax.axis_index("tx")
    ty = lax.axis_index("ty")
    lev = lax.axis_index("lev")
    core = lev % 2
    own_obs, member_count = obs_ref.shape
    blocks = own_obs // 128
    columns = owner_ref.shape[0]
    slots = owner_ref.shape[2]

    def exists(dx, dy):
        x, y = tx + dx, ty + dy
        return (x >= 0) & (x < tiles_x) & (y >= 0) & (y < tiles_y)

    loads = [
        pltpu.make_async_copy(source, target, load_sem.at[k])
        for k, (source, target) in enumerate(
            (
                (obs_ref, obs_v),
                (owner_ref, owner_v),
                (slot_ref, slot_v),
                (count_ref, count_v),
                (local_ref, local_v),
                (precision_ref, scalar_v.at[4, 0]),
                (innovation_ref, scalar_v.at[4, 1]),
                (members_ref, members_v),
            )
        )
    ]
    for load in loads:
        load.start()

    barrier = pltpu.get_barrier_semaphore()
    other_core = (tx, ty, lev + 1 - 2 * core)
    other_chip = (tx, ty, (lev + 2) % 4)
    far_core = (tx, ty, 3 - lev)
    for dx, dy in STEPS:

        @pl.when(exists(dx, dy))
        def _():
            pl.semaphore_signal(
                barrier, inc=1, device_id=(tx + dx, ty + dy, lev), device_id_type=MESH
            )

    outward = 2 * core - 1
    for e in (-1, 0, 1):

        @pl.when(exists(outward, e))
        def _():
            pl.semaphore_signal(
                barrier,
                inc=1,
                device_id=(tx + outward, ty + e, lev + 1 - 2 * core),
                device_id_type=MESH,
            )

    pl.semaphore_signal(barrier, inc=1, device_id=other_core, device_id_type=MESH)
    pl.semaphore_signal(barrier, inc=1, device_id=other_chip, device_id_type=MESH)
    pl.semaphore_signal(barrier, inc=1, device_id=far_core, device_id_type=MESH)

    for dx, dy in STEPS:

        @pl.when(jnp.logical_not(exists(dx, dy)))
        def _():
            near = (1 + dx) * 3 + (1 + dy)
            near_v[near] = jnp.zeros(near_v.shape[1:], BF16)
            scalar_v[near] = jnp.zeros(scalar_v.shape[1:], BF16)

    loads[0].wait()
    near_v[4] = obs_v[...].astype(F32).T.astype(BF16)
    for load in loads[1:7]:
        load.wait()

    reach_x = 1 + (tx > 0).astype(jnp.int32) + (tx < tiles_x - 1).astype(jnp.int32)
    reach_y = 1 + (ty > 0).astype(jnp.int32) + (ty < tiles_y - 1).astype(jnp.int32)
    crossing = exists(outward, 0).astype(jnp.int32) * reach_y
    pl.semaphore_wait(barrier, reach_x * reach_y - 1 + crossing + 3)

    def obs_copies(dx, dy):
        theirs = (1 - dx) * 3 + (1 - dy)
        return tuple(
            pltpu.make_async_remote_copy(
                src_ref=buffer.at[4],
                dst_ref=buffer.at[theirs],
                send_sem=send.at[theirs],
                recv_sem=recv.at[theirs],
                device_id=(tx + dx, ty + dy, lev),
                device_id_type=MESH,
            )
            for buffer, send, recv in (
                (scalar_v, scalar_send, scalar_recv),
                (near_v, obs_send, obs_recv),
            )
        )

    for dx, dy in STEPS:

        @pl.when(exists(dx, dy))
        def _():
            for copy in obs_copies(dx, dy):
                copy.start()

    keys, lanes, parts = [], [], []
    position = lax.broadcasted_iota(jnp.int32, (1, slots), 1)
    quarter = own_obs
    for c in range(columns):
        owner = owner_v[c]
        slot = slot_v[c]
        near_x = owner // tiles_y - tx + 1
        near_y = owner % tiles_y - ty + 1
        block = (near_x * 3 + near_y) * blocks + (slot % quarter) // 128
        live = (position < count_v[:, c : c + 1]) & (slot // quarter == lev)
        keys.append(jnp.where(live, block * 8 + c, -1))
        lanes.append(slot % 128)
        parts.append(local_v[c])
    key = jnp.concatenate(keys, axis=1)
    lane = jnp.concatenate(lanes, axis=1)
    local = jnp.concatenate(parts, axis=1)
    high = local.astype(BF16).astype(F32)
    middle = (local - high).astype(BF16).astype(F32)
    low = local - high - middle
    dense_rows = 9 * blocks * 8
    row = lax.broadcasted_iota(jnp.int32, (dense_rows, columns * slots), 0)
    chosen = row == key
    spot = (lax.broadcasted_iota(jnp.int32, (128, columns * slots), 0) == lane).astype(F32)
    spot = spot.astype(BF16)
    dense = 0.0
    for part in (low, middle, high):
        dense += lax.dot_general(
            jnp.where(chosen, part, 0.0).astype(BF16), spot, NT, preferred_element_type=F32
        )
    dense_v[...] = dense.reshape(9 * blocks, 8, 128)

    gram_v[...] = jnp.zeros_like(gram_v)

    def add_blocks(nears):
        left, right = [], []
        for near in nears:
            turned = near_v[near]
            wide = turned.astype(F32)
            scalars = scalar_v[near].astype(F32)
            weight = jnp.concatenate(
                [dense_v[near * blocks + h] * scalars[0, h : h + 1, :] for h in range(blocks)],
                axis=1,
            )
            departure = jnp.concatenate([scalars[1, h : h + 1, :] for h in range(blocks)], axis=1)
            pairs = [((wide * weight[c : c + 1, :]).astype(BF16),) for c in range(columns)]
            pairs.append(halves(weight * departure))
            left.append(jnp.concatenate([half for pair in pairs for half in pair], axis=0))
            right.append(turned)
        sums = lax.dot_general(
            jnp.concatenate(left, axis=1),
            jnp.concatenate(right, axis=1),
            NT,
            preferred_element_type=F32,
        )
        at = 0
        for c in range(columns):
            gram_v[c, 0:member_count, :] += sums[at : at + member_count]
            at += member_count
        shares = sums[at : at + 8] + sums[at + 8 : at + 16]
        for c in range(columns):
            gram_v[c, member_count : member_count + 8, :] += jnp.broadcast_to(
                shares[c : c + 1, :], (8, member_count)
            )

    add_blocks([4])

    loads[7].wait()
    half_span = SPACING // 2
    averaging = jnp.full((member_count, member_count), 1.0 / member_count, BF16)
    level_count, width_x, width_y, _ = members_v.shape
    for level in range(level_count):
        for first in range(0, width_x, 32):
            states = members_v[level, first : first + 32].reshape(32 * width_y, member_count)
            mean = jnp.dot(states, averaging, preferred_element_type=F32)
            mean_v[level, first : first + 32] = mean.reshape(32, width_y, member_count)
            pert = (states.astype(F32) - mean).reshape(32, width_y, member_count)
            for p in range(2):
                half = pert[:, p * half_span : (p + 1) * half_span].reshape(-1, member_count)
                pert_v[p, level, first * half_span : (first + 32) * half_span] = half.astype(BF16)

    for group in GROUPS:
        for dx, dy in group:

            @pl.when(exists(dx, dy))
            def _():
                for copy in obs_copies(-dx, -dy):
                    copy.wait_recv()

        add_blocks([(1 + dx) * 3 + (1 + dy) for dx, dy in group])

    mine, others = 2 * core, 2 - 2 * core
    for c in range(columns):
        half_v[c, 0:member_count] = gram_v[c, 0:member_count].astype(BF16)
        half_v[c, member_count:] = jnp.concatenate(halves(gram_v[c, member_count:]), axis=0)

    def gram_copy(index, source, target, where):
        return pltpu.make_async_remote_copy(
            src_ref=source,
            dst_ref=target,
            send_sem=gram_send.at[index],
            recv_sem=gram_recv.at[index],
            device_id=where,
            device_id_type=MESH,
        )

    to_core = gram_copy(0, gram_v.at[pl.ds(others, 2)], from_core_v, other_core)
    to_chip = gram_copy(1, half_v.at[pl.ds(mine, 2)], from_chip_v.at[0], other_chip)
    to_far = gram_copy(2, half_v.at[pl.ds(others, 2)], from_chip_v.at[1], far_core)
    to_far.start()
    to_chip.start()
    to_core.start()
    to_core.wait_recv()
    sum_v[...] = gram_v[pl.ds(mine, 2)] + from_core_v[...]
    to_chip.wait_recv()
    to_far.wait_recv()
    for k in range(2):
        theirs = from_chip_v[0, k].astype(F32) + from_chip_v[1, k].astype(F32)
        gram = sum_v[k, 0:member_count] + theirs[0:member_count]
        upper = theirs[member_count : member_count + 8]
        lower = theirs[member_count + 8 : member_count + 16]
        proj = sum_v[k, member_count:] + (upper + lower)
        weights_v[1, 1 + mine + k] = solve(gram, proj)

    rim_from = 1 + 3 * core
    rim_to = 5 - 5 * core

    def pass_copy(index, ref):
        return pltpu.make_async_remote_copy(
            src_ref=ref,
            dst_ref=ref,
            send_sem=pass_send.at[index],
            recv_sem=pass_recv.at[index],
            device_id=other_core,
            device_id_type=MESH,
        )

    def pair(y, first):
        return weights_v.at[y, pl.ds(first, 2)]

    pair_mine, pair_other = 1 + mine, 1 + others
    rim_mine, rim_other = rim_to, 5 - rim_to

    def pair_copy(e):
        return pltpu.make_async_remote_copy(
            src_ref=pair(1, pair_mine),
            dst_ref=pair(1 - e, pair_mine),
            send_sem=weight_send.at[1 - e],
            recv_sem=weight_recv.at[1 - e],
            device_id=(tx, ty + e, lev),
            device_id_type=MESH,
        )

    def rim_copy(e, across):
        where = (tx + outward, ty + e, lev + across * (1 - 2 * core))
        index = 3 + 3 * across + 1 - e
        return pltpu.make_async_remote_copy(
            src_ref=weights_v.at[1, rim_from],
            dst_ref=weights_v.at[1 - e, rim_mine],
            send_sem=weight_send.at[index],
            recv_sem=weight_recv.at[index],
            device_id=where,
            device_id_type=MESH,
        )

    for e in (1, -1):

        @pl.when(exists(0, e))
        def _():
            pair_copy(e).start()

    for e in (1, -1, 0):

        @pl.when(exists(outward, e))
        def _():
            rim_copy(e, 0).start()
            rim_copy(e, 1).start()

    pass_copy(1, pair(1, pair_mine)).start()
    places_y = [jnp.where(ty == 0, 1, 0), 1, jnp.where(ty == tiles_y - 1, 1, 2)]
    places_x = [jnp.where(tx == 0, 1, 0), 1, 2, 3, 4, jnp.where(tx == tiles_x - 1, 4, 5)]
    patches = width_x // half_span
    within = lax.broadcasted_iota(jnp.int32, (half_span, member_count), 0).astype(F32)
    upper_y = [(within + half_span + 0.5) / SPACING, (within + 0.5) / SPACING]
    centre_y = [upper_y[0], 1.0 - upper_y[1]]
    outer_y = [1.0 - upper_y[0], upper_y[1]]

    def part_x(patch, x, u):
        fx = (x + 0.5 + (half_span if patch % 2 == 0 else 0)) / SPACING
        return fx if u else 1.0 - fx

    def mix(patch, p, places):
        first = patch * half_span * half_span
        states = pert_v[p, :, first : first + half_span * half_span].reshape(-1, member_count)
        corners = jnp.concatenate([weights_v[y, x] for y, x in places], axis=1)
        mixed = jnp.dot(states, corners, preferred_element_type=F32)
        return mixed.reshape(level_count, half_span, half_span, len(places) * member_count)

    def add_centre(patch):
        left = (patch + 1) // 2
        sides = [u for u in range(2) if 1 <= left + u <= 4]
        for p in range(2):
            mixed = mix(patch, p, [(1, left + u) for u in sides])
            for level in range(level_count):
                for x in range(half_span):
                    at = (level, patch * half_span + x, slice(p * half_span, (p + 1) * half_span))
                    total = mean_v[at]
                    for i, u in enumerate(sides):
                        share = mixed[level, x, :, i * member_count : (i + 1) * member_count]
                        total = total + share * (part_x(patch, x, u) * centre_y[p])
                    mean_v[at] = total

    def finish(patch):
        left = (patch + 1) // 2
        rims = [u for u in range(2) if not 1 <= left + u <= 4]
        mixed = [
            mix(
                patch,
                p,
                [(places_y[2 * p], places_x[left + u]) for u in range(2)]
                + [(1, places_x[left + u]) for u in rims],
            )
            for p in range(2)
        ]
        for level in range(level_count):
            for x in range(half_span):
                sides = []
                for p in range(2):
                    total = mean_v[
                        level, patch * half_span + x, p * half_span : (p + 1) * half_span
                    ]
                    factors = [part_x(patch, x, u) * outer_y[p] for u in range(2)]
                    factors += [part_x(patch, x, u) * centre_y[p] for u in rims]
                    for i, factor in enumerate(factors):
                        share = mixed[p][level, x, :, i * member_count : (i + 1) * member_count]
                        total = total + share * factor
                    sides.append(total)
                out_ref[level, patch * half_span + x] = jnp.concatenate(sides, axis=0).astype(BF16)

    pass_copy(1, pair(1, pair_other)).wait_recv()
    for patch in range(patches):
        add_centre(patch)

    for e in (1, -1):

        @pl.when(exists(0, -e))
        def _():
            pair_copy(e).wait_recv()
            pass_copy(1 - e, pair(1 - e, pair_mine)).start()

    for e in (1, -1):

        @pl.when(exists(0, -e))
        def _():
            pass_copy(1 - e, pair(1 - e, pair_other)).wait_recv()

    for patch in range(1, patches - 1):
        finish(patch)

    for e in (0, 1, -1):

        @pl.when(exists(-outward, -e))
        def _():
            rim_copy(e, 0).wait_recv()

        @pl.when(exists(outward, -e))
        def _():
            pltpu.make_async_remote_copy(
                src_ref=weights_v.at[1, rim_from],
                dst_ref=weights_v.at[1 - e, rim_other],
                send_sem=weight_send.at[7 - e],
                recv_sem=weight_recv.at[7 - e],
                device_id=other_core,
                device_id_type=MESH,
            ).wait_recv()

    finish(0)
    finish(patches - 1)

    for dx, dy in STEPS:

        @pl.when(exists(dx, dy))
        def _():
            for copy in obs_copies(dx, dy):
                copy.wait_send()

    to_core.wait_send()
    to_chip.wait_send()
    to_far.wait_send()
    pass_copy(1, pair(1, pair_mine)).wait_send()
    for e in (0, 1, -1):
        if e:

            @pl.when(exists(0, e))
            def _():
                pair_copy(e).wait_send()

            @pl.when(exists(0, -e))
            def _():
                pass_copy(1 - e, pair(1 - e, pair_mine)).wait_send()

        @pl.when(exists(outward, e))
        def _():
            rim_copy(e, 0).wait_send()
            rim_copy(e, 1).wait_send()


def per_device(
    tiles_x,
    tiles_y,
    members,
    obs_pert,
    innovation,
    obs_precision,
    obs_owner,
    obs_slot,
    obs_count,
    local_weight,
):
    own_obs, member_count = obs_pert.shape
    blocks = own_obs // 128
    anywhere = pl.BlockSpec(memory_space=pltpu.HBM)
    dma = pltpu.SemaphoreType.DMA
    return pl.pallas_call(
        functools.partial(kernel, tiles_x, tiles_y),
        out_shape=jax.ShapeDtypeStruct(members.shape, BF16),
        in_specs=[anywhere] * 8,
        out_specs=pl.BlockSpec(memory_space=pltpu.VMEM),
        scratch_shapes=[
            pltpu.VMEM(members.shape, BF16),
            pltpu.VMEM((2, members.shape[0], members.shape[1] * SPACING // 2, member_count), BF16),
            pltpu.VMEM(members.shape, F32),
            pltpu.VMEM(obs_pert.shape, BF16),
            pltpu.VMEM((9, member_count, own_obs), BF16),
            pltpu.VMEM((9, 2, blocks, 128), BF16),
            pltpu.VMEM(obs_owner.shape, jnp.int32),
            pltpu.VMEM(obs_slot.shape, jnp.int32),
            pltpu.VMEM((1, obs_count.size), jnp.int32),
            pltpu.VMEM(local_weight.shape, F32),
            pltpu.VMEM((9 * blocks, 8, 128), F32),
            pltpu.VMEM((4, member_count + 8, member_count), F32),
            pltpu.VMEM((2, member_count + 8, member_count), F32),
            pltpu.VMEM((2, member_count + 8, member_count), F32),
            pltpu.VMEM((4, member_count + 16, member_count), BF16),
            pltpu.VMEM((2, 2, member_count + 16, member_count), BF16),
            pltpu.VMEM((3, 6, member_count, member_count), BF16),
            dma((8,)),
            dma((9,)),
            dma((9,)),
            dma((9,)),
            dma((9,)),
            dma((3,)),
            dma((3,)),
            dma((9,)),
            dma((9,)),
            dma((3,)),
            dma((3,)),
        ],
        compiler_params=pltpu.CompilerParams(
            collective_id=0, has_side_effects=True, vmem_limit_bytes=48 * 1024 * 1024
        ),
    )(
        *(pltpu.with_memory_space_constraint(x, pltpu.HBM) for x in (
        members,
        obs_pert,
        innovation.reshape(blocks, 128),
        obs_precision.reshape(blocks, 128),
        obs_owner,
        obs_slot,
        obs_count.reshape(1, -1),
        local_weight,
        ))
    )


def solution(mesh):
    placed = (
        P("lev", "tx", "ty", None),
        P(("tx", "ty", "lev"), None),
        P(("tx", "ty", "lev")),
        P(("tx", "ty", "lev")),
        P("tx", "ty", None),
        P("tx", "ty", None),
        P("tx", "ty"),
        P("tx", "ty", None),
    )
    return jax.shard_map(
        functools.partial(per_device, mesh.shape["tx"], mesh.shape["ty"]),
        mesh=mesh,
        in_specs=placed,
        out_specs=P("lev", "tx", "ty", None),
        check_vma=False,
    )
```

```python
import functools

import jax
import jax.numpy as jnp
from jax import lax
from jax.experimental import pallas as pl
from jax.experimental.pallas import tpu as pltpu
from jax.sharding import PartitionSpec as P

SPACING = 16
NS_STEPS = 4
MESH = pl.DeviceIdType.MESH
F32 = jnp.float32
BF16 = jnp.bfloat16
NT = (((1,), (1,)), ((), ()))

STEPS = ((1, 1), (1, -1), (-1, 1), (-1, -1), (0, 1), (0, -1), (1, 0), (-1, 0))
GROUPS = (STEPS,)


def halves(value):
    high = value.astype(BF16)
    return high, (value - high.astype(F32)).astype(BF16)


def product(left, right):
    left_high, left_low = left
    right_high, right_low = right
    return jnp.dot(
        jnp.concatenate([left_high, left_high, left_low], axis=1),
        jnp.concatenate([right_high, right_low, right_high], axis=0),
        preferred_element_type=F32,
    )


def beside(left, right):
    return tuple(jnp.concatenate(pair, axis=1) for pair in zip(left, right))


def products(lefts, rights):
    return [product(left, right) for left, right in zip(lefts, rights)]


def split(values):
    return [halves(value) for value in values]


def solve(grams, proj_rows):
    shape = grams[0].shape
    members = shape[0]
    spread = float(members - 1)
    rows = lax.broadcasted_iota(jnp.int32, shape, 0)
    columns = lax.broadcasted_iota(jnp.int32, shape, 1)
    diagonal = rows == columns
    three_halves = jnp.where(diagonal, 1.5, 0.0)
    raised = [jnp.where(diagonal, spread, 0.0) + gram for gram in grams]
    split_raised = split(raised)
    squares = [
        jnp.sum(jnp.sum(gram * gram, axis=0, keepdims=True), axis=1, keepdims=True)
        for gram in grams
    ]
    squared = products(split_raised, split_raised)
    norms = [spread + jnp.sqrt(square) for square in squares]
    scales = [1.0 / norm for norm in norms]
    bases = [value * scale for value, scale in zip(raised, scales)]
    inverses = [three_halves - 0.5 * base for base in bases]
    roots = [
        1.5 * base - square * (0.5 * scale * scale)
        for base, square, scale in zip(bases, squared, scales)
    ]
    targets = [jnp.broadcast_to(proj[0:1, :], shape).T for proj in proj_rows]
    for step in range(1, NS_STEPS):
        split_inverses, split_roots = split(inverses), split(roots)
        if step < NS_STEPS - 1:
            between = products(split_inverses, split_roots)
            middles = [three_halves - 0.5 * value for value in between]
            seconds = [beside(r, i) for r, i in zip(split_roots, split_inverses)]
            both = products(split(middles), seconds)
            roots = [value[:, :members] for value in both]
            inverses = [value[:, members:] for value in both]
        else:
            seconds = [beside(r, t) for r, t in zip(split_roots, split(targets))]
            both = products(split_inverses, seconds)
            middles = [three_halves - 0.5 * value[:, :members] for value in both]
            mapped = split([value[:, members:] for value in both])
            seconds = [beside(i, t) for i, t in zip(split_inverses, mapped)]
            both = products(split(middles), seconds)
            inverses = [value[:, :members] for value in both]
            inners = [value[:, members:] for value in both]
    means = products(split(inverses), split(inners))
    return [
        ((jnp.sqrt(spread) * lax.rsqrt(norm)) * inverse + mean * scale).astype(BF16)
        for norm, inverse, mean, scale in zip(norms, inverses, means, scales)
    ]


def kernel(
    tiles_x,
    tiles_y,
    members_ref,
    obs_ref,
    innovation_ref,
    precision_ref,
    owner_ref,
    slot_ref,
    count_ref,
    local_ref,
    out_ref,
    members_v,
    pert_v,
    mean_v,
    obs_v,
    near_v,
    scalar_v,
    owner_v,
    slot_v,
    count_v,
    local_v,
    dense_v,
    gram_v,
    from_core_v,
    sum_v,
    half_v,
    from_chip_v,
    weights_v,
    load_sem,
    obs_send,
    obs_recv,
    scalar_send,
    scalar_recv,
    gram_send,
    gram_recv,
    weight_send,
    weight_recv,
    pass_send,
    pass_recv,
):
    tx = lax.axis_index("tx")
    ty = lax.axis_index("ty")
    lev = lax.axis_index("lev")
    core = lev % 2
    own_obs, member_count = obs_ref.shape
    blocks = own_obs // 128
    columns = owner_ref.shape[0]
    slots = owner_ref.shape[2]

    def exists(dx, dy):
        x, y = tx + dx, ty + dy
        return (x >= 0) & (x < tiles_x) & (y >= 0) & (y < tiles_y)

    loads = [
        pltpu.make_async_copy(source, target, load_sem.at[k])
        for k, (source, target) in enumerate(
            (
                (obs_ref, obs_v),
                (owner_ref, owner_v),
                (slot_ref, slot_v),
                (count_ref, count_v),
                (local_ref, local_v),
                (precision_ref, scalar_v.at[4, 0]),
                (innovation_ref, scalar_v.at[4, 1]),
                (members_ref, members_v),
            )
        )
    ]
    for load in loads:
        load.start()

    barrier = pltpu.get_barrier_semaphore()
    other_core = (tx, ty, lev + 1 - 2 * core)
    other_chip = (tx, ty, (lev + 2) % 4)
    far_core = (tx, ty, 3 - lev)
    for dx, dy in STEPS:

        @pl.when(exists(dx, dy))
        def _():
            pl.semaphore_signal(
                barrier, inc=1, device_id=(tx + dx, ty + dy, lev), device_id_type=MESH
            )

    outward = 2 * core - 1
    for e in (-1, 0, 1):

        @pl.when(exists(outward, e))
        def _():
            pl.semaphore_signal(
                barrier,
                inc=1,
                device_id=(tx + outward, ty + e, lev + 1 - 2 * core),
                device_id_type=MESH,
            )

    pl.semaphore_signal(barrier, inc=1, device_id=other_core, device_id_type=MESH)
    pl.semaphore_signal(barrier, inc=1, device_id=other_chip, device_id_type=MESH)
    pl.semaphore_signal(barrier, inc=1, device_id=far_core, device_id_type=MESH)

    for dx, dy in STEPS:

        @pl.when(jnp.logical_not(exists(dx, dy)))
        def _():
            near = (1 + dx) * 3 + (1 + dy)
            near_v[near] = jnp.zeros(near_v.shape[1:], BF16)
            scalar_v[near] = jnp.zeros(scalar_v.shape[1:], BF16)

    loads[0].wait()
    near_v[4] = obs_v[...].astype(F32).T.astype(BF16)
    for load in loads[1:7]:
        load.wait()

    reach_x = 1 + (tx > 0).astype(jnp.int32) + (tx < tiles_x - 1).astype(jnp.int32)
    reach_y = 1 + (ty > 0).astype(jnp.int32) + (ty < tiles_y - 1).astype(jnp.int32)
    crossing = exists(outward, 0).astype(jnp.int32) * reach_y
    pl.semaphore_wait(barrier, reach_x * reach_y - 1 + crossing + 3)

    def obs_copies(dx, dy):
        theirs = (1 - dx) * 3 + (1 - dy)
        return tuple(
            pltpu.make_async_remote_copy(
                src_ref=buffer.at[4],
                dst_ref=buffer.at[theirs],
                send_sem=send.at[theirs],
                recv_sem=recv.at[theirs],
                device_id=(tx + dx, ty + dy, lev),
                device_id_type=MESH,
            )
            for buffer, send, recv in (
                (scalar_v, scalar_send, scalar_recv),
                (near_v, obs_send, obs_recv),
            )
        )

    for dx, dy in STEPS:

        @pl.when(exists(dx, dy))
        def _():
            for copy in obs_copies(dx, dy):
                copy.start()

    keys, lanes, parts = [], [], []
    position = lax.broadcasted_iota(jnp.int32, (1, slots), 1)
    quarter = own_obs
    for c in range(columns):
        owner = owner_v[c]
        slot = slot_v[c]
        near_x = owner // tiles_y - tx + 1
        near_y = owner % tiles_y - ty + 1
        block = (near_x * 3 + near_y) * blocks + (slot % quarter) // 128
        live = (position < count_v[:, c : c + 1]) & (slot // quarter == lev)
        keys.append(jnp.where(live, block * 8 + c, -1))
        lanes.append(slot % 128)
        parts.append(local_v[c])
    key = jnp.concatenate(keys, axis=1)
    lane = jnp.concatenate(lanes, axis=1)
    local = jnp.concatenate(parts, axis=1)
    high = local.astype(BF16).astype(F32)
    middle = (local - high).astype(BF16).astype(F32)
    low = local - high - middle
    dense_rows = 9 * blocks * 8
    row = lax.broadcasted_iota(jnp.int32, (dense_rows, columns * slots), 0)
    chosen = row == key
    spot = (lax.broadcasted_iota(jnp.int32, (128, columns * slots), 0) == lane).astype(F32)
    spot = spot.astype(BF16)
    dense = 0.0
    for part in (low, middle, high):
        dense += lax.dot_general(
            jnp.where(chosen, part, 0.0).astype(BF16), spot, NT, preferred_element_type=F32
        )
    dense_v[...] = dense.reshape(9 * blocks, 8, 128)

    gram_v[...] = jnp.zeros_like(gram_v)

    def add_blocks(nears):
        left, right = [], []
        for near in nears:
            turned = near_v[near]
            wide = turned.astype(F32)
            scalars = scalar_v[near].astype(F32)
            weight = jnp.concatenate(
                [dense_v[near * blocks + h] * scalars[0, h : h + 1, :] for h in range(blocks)],
                axis=1,
            )
            departure = jnp.concatenate([scalars[1, h : h + 1, :] for h in range(blocks)], axis=1)
            pairs = [((wide * weight[c : c + 1, :]).astype(BF16),) for c in range(columns)]
            pairs.append(halves(weight * departure))
            left.append(jnp.concatenate([half for pair in pairs for half in pair], axis=0))
            right.append(turned)
        sums = lax.dot_general(
            jnp.concatenate(left, axis=1),
            jnp.concatenate(right, axis=1),
            NT,
            preferred_element_type=F32,
        )
        at = 0
        for c in range(columns):
            gram_v[c, 0:member_count, :] += sums[at : at + member_count]
            at += member_count
        shares = sums[at : at + 8] + sums[at + 8 : at + 16]
        for c in range(columns):
            gram_v[c, member_count : member_count + 8, :] += jnp.broadcast_to(
                shares[c : c + 1, :], (8, member_count)
            )

    add_blocks([4])

    loads[7].wait()
    half_span = SPACING // 2
    averaging = jnp.full((member_count, member_count), 1.0 / member_count, BF16)
    level_count, width_x, width_y, _ = members_v.shape
    for level in range(level_count):
        for first in range(0, width_x, 32):
            states = members_v[level, first : first + 32].reshape(32 * width_y, member_count)
            mean = jnp.dot(states, averaging, preferred_element_type=F32)
            mean_v[level, first : first + 32] = mean.reshape(32, width_y, member_count)
            pert = (states.astype(F32) - mean).reshape(32, width_y, member_count)
            for p in range(2):
                half = pert[:, p * half_span : (p + 1) * half_span].reshape(-1, member_count)
                pert_v[p, level, first * half_span : (first + 32) * half_span] = half.astype(BF16)

    for group in GROUPS:
        for dx, dy in group:

            @pl.when(exists(dx, dy))
            def _():
                for copy in obs_copies(-dx, -dy):
                    copy.wait_recv()

        add_blocks([(1 + dx) * 3 + (1 + dy) for dx, dy in group])

    mine, others = 2 * core, 2 - 2 * core
    for c in range(columns):
        half_v[c, 0:member_count] = gram_v[c, 0:member_count].astype(BF16)
        half_v[c, member_count:] = jnp.concatenate(halves(gram_v[c, member_count:]), axis=0)

    def gram_copy(index, source, target, where):
        return pltpu.make_async_remote_copy(
            src_ref=source,
            dst_ref=target,
            send_sem=gram_send.at[index],
            recv_sem=gram_recv.at[index],
            device_id=where,
            device_id_type=MESH,
        )

    to_core = gram_copy(0, gram_v.at[pl.ds(others, 2)], from_core_v, other_core)
    to_chip = gram_copy(1, half_v.at[pl.ds(mine, 2)], from_chip_v.at[0], other_chip)
    to_far = gram_copy(2, half_v.at[pl.ds(others, 2)], from_chip_v.at[1], far_core)
    to_far.start()
    to_chip.start()
    to_core.start()
    to_core.wait_recv()
    sum_v[...] = gram_v[pl.ds(mine, 2)] + from_core_v[...]
    to_chip.wait_recv()
    to_far.wait_recv()
    grams, projs = [], []
    for k in range(2):
        theirs = from_chip_v[0, k].astype(F32) + from_chip_v[1, k].astype(F32)
        gram = sum_v[k, 0:member_count] + theirs[0:member_count]
        upper = theirs[member_count : member_count + 8]
        lower = theirs[member_count + 8 : member_count + 16]
        proj = sum_v[k, member_count:] + (upper + lower)
        grams.append(gram)
        projs.append(proj)
    for k, weights in enumerate(solve(grams, projs)):
        weights_v[1, 1 + mine + k] = weights

    rim_from = 1 + 3 * core
    rim_to = 5 - 5 * core

    def pass_copy(index, ref):
        return pltpu.make_async_remote_copy(
            src_ref=ref,
            dst_ref=ref,
            send_sem=pass_send.at[index],
            recv_sem=pass_recv.at[index],
            device_id=other_core,
            device_id_type=MESH,
        )

    def pair(y, first):
        return weights_v.at[y, pl.ds(first, 2)]

    pair_mine, pair_other = 1 + mine, 1 + others
    rim_mine, rim_other = rim_to, 5 - rim_to

    def pair_copy(e):
        return pltpu.make_async_remote_copy(
            src_ref=pair(1, pair_mine),
            dst_ref=pair(1 - e, pair_mine),
            send_sem=weight_send.at[1 - e],
            recv_sem=weight_recv.at[1 - e],
            device_id=(tx, ty + e, lev),
            device_id_type=MESH,
        )

    def rim_copy(e, across):
        where = (tx + outward, ty + e, lev + across * (1 - 2 * core))
        index = 3 + 3 * across + 1 - e
        return pltpu.make_async_remote_copy(
            src_ref=weights_v.at[1, rim_from],
            dst_ref=weights_v.at[1 - e, rim_mine],
            send_sem=weight_send.at[index],
            recv_sem=weight_recv.at[index],
            device_id=where,
            device_id_type=MESH,
        )

    for e in (1, -1):

        @pl.when(exists(0, e))
        def _():
            pair_copy(e).start()

    for e in (1, -1, 0):

        @pl.when(exists(outward, e))
        def _():
            rim_copy(e, 0).start()
            rim_copy(e, 1).start()

    pass_copy(1, pair(1, pair_mine)).start()
    places_y = [jnp.where(ty == 0, 1, 0), 1, jnp.where(ty == tiles_y - 1, 1, 2)]
    places_x = [jnp.where(tx == 0, 1, 0), 1, 2, 3, 4, jnp.where(tx == tiles_x - 1, 4, 5)]
    patches = width_x // half_span
    within = lax.broadcasted_iota(jnp.int32, (half_span, member_count), 0).astype(F32)
    upper_y = [(within + half_span + 0.5) / SPACING, (within + 0.5) / SPACING]
    centre_y = [upper_y[0], 1.0 - upper_y[1]]
    outer_y = [1.0 - upper_y[0], upper_y[1]]

    def part_x(patch, x, u):
        fx = (x + 0.5 + (half_span if patch % 2 == 0 else 0)) / SPACING
        return fx if u else 1.0 - fx

    def mix(patch, p, places):
        first = patch * half_span * half_span
        states = pert_v[p, :, first : first + half_span * half_span].reshape(-1, member_count)
        corners = jnp.concatenate([weights_v[y, x] for y, x in places], axis=1)
        mixed = jnp.dot(states, corners, preferred_element_type=F32)
        return mixed.reshape(level_count, half_span, half_span, len(places) * member_count)

    def add_centre(patch):
        left = (patch + 1) // 2
        sides = [u for u in range(2) if 1 <= left + u <= 4]
        for p in range(2):
            mixed = mix(patch, p, [(1, left + u) for u in sides])
            for level in range(level_count):
                for x in range(half_span):
                    at = (level, patch * half_span + x, slice(p * half_span, (p + 1) * half_span))
                    total = mean_v[at]
                    for i, u in enumerate(sides):
                        share = mixed[level, x, :, i * member_count : (i + 1) * member_count]
                        total = total + share * (part_x(patch, x, u) * centre_y[p])
                    mean_v[at] = total

    def finish(patch):
        left = (patch + 1) // 2
        rims = [u for u in range(2) if not 1 <= left + u <= 4]
        mixed = [
            mix(
                patch,
                p,
                [(places_y[2 * p], places_x[left + u]) for u in range(2)]
                + [(1, places_x[left + u]) for u in rims],
            )
            for p in range(2)
        ]
        for level in range(level_count):
            for x in range(half_span):
                sides = []
                for p in range(2):
                    total = mean_v[
                        level, patch * half_span + x, p * half_span : (p + 1) * half_span
                    ]
                    factors = [part_x(patch, x, u) * outer_y[p] for u in range(2)]
                    factors += [part_x(patch, x, u) * centre_y[p] for u in rims]
                    for i, factor in enumerate(factors):
                        share = mixed[p][level, x, :, i * member_count : (i + 1) * member_count]
                        total = total + share * factor
                    sides.append(total)
                out_ref[level, patch * half_span + x] = jnp.concatenate(sides, axis=0).astype(BF16)

    pass_copy(1, pair(1, pair_other)).wait_recv()
    for patch in range(patches):
        add_centre(patch)

    for e in (1, -1):

        @pl.when(exists(0, -e))
        def _():
            pair_copy(e).wait_recv()
            pass_copy(1 - e, pair(1 - e, pair_mine)).start()

    for e in (1, -1):

        @pl.when(exists(0, -e))
        def _():
            pass_copy(1 - e, pair(1 - e, pair_other)).wait_recv()

    for patch in range(1, patches - 1):
        finish(patch)

    for e in (0, 1, -1):

        @pl.when(exists(-outward, -e))
        def _():
            rim_copy(e, 0).wait_recv()

        @pl.when(exists(outward, -e))
        def _():
            pltpu.make_async_remote_copy(
                src_ref=weights_v.at[1, rim_from],
                dst_ref=weights_v.at[1 - e, rim_other],
                send_sem=weight_send.at[7 - e],
                recv_sem=weight_recv.at[7 - e],
                device_id=other_core,
                device_id_type=MESH,
            ).wait_recv()

    finish(0)
    finish(patches - 1)

    for dx, dy in STEPS:

        @pl.when(exists(dx, dy))
        def _():
            for copy in obs_copies(dx, dy):
                copy.wait_send()

    to_core.wait_send()
    to_chip.wait_send()
    to_far.wait_send()
    pass_copy(1, pair(1, pair_mine)).wait_send()
    for e in (0, 1, -1):
        if e:

            @pl.when(exists(0, e))
            def _():
                pair_copy(e).wait_send()

            @pl.when(exists(0, -e))
            def _():
                pass_copy(1 - e, pair(1 - e, pair_mine)).wait_send()

        @pl.when(exists(outward, e))
        def _():
            rim_copy(e, 0).wait_send()
            rim_copy(e, 1).wait_send()


def per_device(
    tiles_x,
    tiles_y,
    members,
    obs_pert,
    innovation,
    obs_precision,
    obs_owner,
    obs_slot,
    obs_count,
    local_weight,
):
    own_obs, member_count = obs_pert.shape
    blocks = own_obs // 128
    anywhere = pl.BlockSpec(memory_space=pltpu.HBM)
    dma = pltpu.SemaphoreType.DMA
    return pl.pallas_call(
        functools.partial(kernel, tiles_x, tiles_y),
        out_shape=jax.ShapeDtypeStruct(members.shape, BF16),
        in_specs=[anywhere] * 8,
        out_specs=pl.BlockSpec(memory_space=pltpu.VMEM),
        scratch_shapes=[
            pltpu.VMEM(members.shape, BF16),
            pltpu.VMEM((2, members.shape[0], members.shape[1] * SPACING // 2, member_count), BF16),
            pltpu.VMEM(members.shape, F32),
            pltpu.VMEM(obs_pert.shape, BF16),
            pltpu.VMEM((9, member_count, own_obs), BF16),
            pltpu.VMEM((9, 2, blocks, 128), BF16),
            pltpu.VMEM(obs_owner.shape, jnp.int32),
            pltpu.VMEM(obs_slot.shape, jnp.int32),
            pltpu.VMEM((1, obs_count.size), jnp.int32),
            pltpu.VMEM(local_weight.shape, F32),
            pltpu.VMEM((9 * blocks, 8, 128), F32),
            pltpu.VMEM((4, member_count + 8, member_count), F32),
            pltpu.VMEM((2, member_count + 8, member_count), F32),
            pltpu.VMEM((2, member_count + 8, member_count), F32),
            pltpu.VMEM((4, member_count + 16, member_count), BF16),
            pltpu.VMEM((2, 2, member_count + 16, member_count), BF16),
            pltpu.VMEM((3, 6, member_count, member_count), BF16),
            dma((8,)),
            dma((9,)),
            dma((9,)),
            dma((9,)),
            dma((9,)),
            dma((3,)),
            dma((3,)),
            dma((9,)),
            dma((9,)),
            dma((3,)),
            dma((3,)),
        ],
        compiler_params=pltpu.CompilerParams(
            collective_id=0, has_side_effects=True, vmem_limit_bytes=48 * 1024 * 1024
        ),
    )(
        *(pltpu.with_memory_space_constraint(x, pltpu.HBM) for x in (
        members,
        obs_pert,
        innovation.reshape(blocks, 128),
        obs_precision.reshape(blocks, 128),
        obs_owner,
        obs_slot,
        obs_count.reshape(1, -1),
        local_weight,
        ))
    )


def solution(mesh):
    placed = (
        P("lev", "tx", "ty", None),
        P(("tx", "ty", "lev"), None),
        P(("tx", "ty", "lev")),
        P(("tx", "ty", "lev")),
        P("tx", "ty", None),
        P("tx", "ty", None),
        P("tx", "ty"),
        P("tx", "ty", None),
    )
    return jax.shard_map(
        functools.partial(per_device, mesh.shape["tx"], mesh.shape["ty"]),
        mesh=mesh,
        in_specs=placed,
        out_specs=P("lev", "tx", "ty", None),
        check_vma=False,
    )
```
